16 devices in a mesh: dp: 4 (over y, z, core), sp: 4 (over x).
Axes of the slice: x: 4, y: 2, z: 1, core: 2. Of those that a mesh axis runs over, the one named last changes fastest.
The devices are a block of a 4x4x8 slice.
Arguments:
- x: bfloat16 [16384, 4096], P(('dp', 'sp')), parts along dimension 0
- gain: bfloat16 [4096], replicated
- wq: bfloat16 [4096, 4096], P('sp')
- wk: bfloat16 [4096, 512], P('sp')
- wv: bfloat16 [4096, 512], P('sp')
- wo: bfloat16 [4096, 4096], P('sp')
Outputs:
- output: bfloat16 [16384, 4096], P(('dp', 'sp')), parts along dimension 0
There are 4 independent parts. The reference program is written for one: setup_inputs(seed, part) draws one part's arguments, and reference() takes and returns one part's arrays. A program takes and returns all parts, laid end to end along the dimension named above; an argument that names none is the same for every part.
All inputs are finite; a program needn't handle non-finite values.
Results may differ from the reference program's by a relative error of at most 0.012.
Values are sent between devices in bfloat16 or wider.
A program may use at most 768 MiB of HBM per device.

```python
import jax
import jax.numpy as jnp
from jax import lax

ROWS = 4096
D = 4096
HEADS = 32
KV_HEADS = 4
HEAD = 128
THETA = 10000


def setup_inputs(seed: int = 0, part: int = 0) -> dict:
    kx, kn, kq, kk, kv, ko = jax.random.split(jax.random.key(seed), 6)

    def weights(key, rows, columns):
        return jax.random.normal(key, (rows, columns), jnp.float32) * rows**-0.5

    drawn = {
        "x": jax.random.normal(jax.random.fold_in(kx, part), (ROWS, D), jnp.float32),
        "gain": 1 + 0.1 * jax.random.normal(kn, (D,), jnp.float32),
        "wq": 2 * weights(kq, D, HEADS * HEAD),
        "wk": 2 * weights(kk, D, KV_HEADS * HEAD),
        "wv": 4 * weights(kv, D, KV_HEADS * HEAD),
        "wo": weights(ko, HEADS * HEAD, D),
    }
    return {k: v.astype(jnp.bfloat16) for k, v in drawn.items()}


def normed(x, gain):
    wide = x.astype(jnp.float32)
    scale = lax.rsqrt(jnp.mean(wide * wide, -1, keepdims=True) + 1e-6)
    return (wide * scale * gain.astype(jnp.float32)).astype(jnp.bfloat16)


def turned(t, place, theta):
    half = t.shape[-1] // 2
    angle = place.astype(jnp.float32)[:, None] * theta ** (-jnp.arange(half, dtype=jnp.float32) / half)
    cos, sin = jnp.cos(angle)[:, None], jnp.sin(angle)[:, None]
    a, b = t[..., :half].astype(jnp.float32), t[..., half:].astype(jnp.float32)
    return jnp.concatenate([a * cos - b * sin, b * cos + a * sin], -1).astype(jnp.bfloat16)


def matmul(a, w):
    return jnp.dot(a, w, preferred_element_type=jnp.float32).astype(jnp.bfloat16)


def einsum(form, a, b):
    return jnp.einsum(form, a.astype(jnp.float32), b.astype(jnp.float32))


def attention(q, k, v):
    scores = einsum("tgsd,ugd->gstu", q, k) * q.shape[-1] ** -0.5
    token = jnp.arange(q.shape[0])
    scores = jnp.where(token[:, None] >= token, scores, -jnp.inf)
    weights = jax.nn.softmax(scores, -1).astype(jnp.bfloat16)
    return einsum("gstu,ugd->tgsd", weights, v).astype(jnp.bfloat16)


def reference(x, gain, wq, wk, wv, wo):
    a, place = normed(x, gain), jnp.arange(ROWS)
    q = turned(matmul(a, wq).reshape(ROWS, HEADS, HEAD), place, THETA).reshape(ROWS, KV_HEADS, -1, HEAD)
    k = turned(matmul(a, wk).reshape(ROWS, KV_HEADS, HEAD), place, THETA)
    v = matmul(a, wv).reshape(ROWS, KV_HEADS, HEAD)
    seen = attention(q, k, v).reshape(ROWS, HEADS * HEAD)
    return (x.astype(jnp.float32) + jnp.dot(seen, wo, preferred_element_type=jnp.float32)).astype(jnp.bfloat16)
```

```python
import functools

import jax
import jax.numpy as jnp
from jax import lax
from jax.experimental import pallas as pl
from jax.experimental.pallas import tpu as pltpu
from jax.sharding import PartitionSpec as P

HEAD = 128
THETA = 10000
NEG = -1e30
HIDDEN = 2 * NEG
LOG2E = 1.4426950408889634
TILE = 512
CHUNK = 256
BQ = 512
BK = 512
SEG = 4
MESH = pl.DeviceIdType.MESH
AHEAD = 2


def _dot(a, b, ca, cb):
    return lax.dot_general(a, b, (((ca,), (cb,)), ((), ())), preferred_element_type=jnp.float32)


def _kernel(n, nq, no, g, x_ref, gain_ref, cos_ref, sin_ref, wq_ref, wk_ref, wv_ref, wo_ref, y_ref, full_ref,
            a_s, o_s, kv_s, w_s, q_s, mix_s, top_s, gap_s, xt_s, yt_s,
            send, recv, kv_send, kv_recv, load_sem, x_sem, y_sem, in_sem):
    me, dp = lax.axis_index("sp"), lax.axis_index("dp")
    rows = x_ref.shape[0]
    part = wq_ref.shape[0]
    kvh = kv_s.shape[0]
    blocks = 2 + nq + no
    right, left, far = lax.rem(me + 1, n), lax.rem(me + n - 1, n), lax.rem(me + 2, n)
    core, pair = lax.rem(dp, 2), lax.rem(lax.div(dp, 2), 2)
    at_right, at_left = {"sp": right}, {"sp": left}
    at_core, at_pair = {"dp": dp + 1 - 2 * core}, {"dp": dp + 2 - 4 * pair}
    origins = (left, right, far)

    barrier = pltpu.get_barrier_semaphore()
    for there in (at_right, at_left, at_core, at_pair):
        pl.semaphore_signal(barrier, inc=1, device_id=there, device_id_type=MESH)
    x_in = pltpu.make_async_copy(x_ref, o_s, in_sem)
    x_in.start()
    pl.semaphore_wait(barrier, 4)

    def narrow(b):
        return (b == 0) | (b == 2) | (b == blocks // 2) | (b == blocks - 1)

    def copy(b, i, src, dst, there):
        return pltpu.make_async_remote_copy(src_ref=src, dst_ref=dst, send_sem=send.at[b, i], recv_sem=recv.at[b, i],
                                            device_id=there, device_id_type=MESH)

    def there_and_here(b, i, ref, there):
        return copy(b, i, ref, ref, there)

    def rows_of(b, origin, start, count):
        return full_ref.at[b, pl.ds(pl.multiple_of(origin * part + start, 128), count), :]

    def both(b, do):
        @pl.when(narrow(b))
        def _():
            do(part // 2, core * (part // 2), True)

        @pl.when(jnp.logical_not(narrow(b)))
        def _():
            do(part // 4, (2 * pair + core) * (part // 4), False)

    def stage0(b):
        def do(count, start, _):
            def go(src, col):
                own = src.at[pl.ds(pl.multiple_of(start, 128), count), pl.ds(pl.multiple_of(col * TILE, TILE), TILE)]
                copy(b, 0, own, rows_of(b, me, start, count), at_right).start()
                copy(b, 1, own, rows_of(b, me, start, count), at_left).start()

            pl.when(b == 0)(lambda: go(wk_ref, 0))
            pl.when(b == 1)(lambda: go(wv_ref, 0))
            pl.when((b >= 2) & (b < 2 + nq))(lambda: go(wq_ref, b - 2))
            pl.when(b >= 2 + nq)(lambda: go(wo_ref, b - 2 - nq))

        both(b, do)

    def onward(b, origin, k, start, count, is_narrow):
        ref = rows_of(b, origin, start, count)
        if not is_narrow:
            there_and_here(b, 4 + k, ref, at_pair).start()
        there_and_here(b, 7 + k, ref, at_core).start()

    def stage1(b):
        def do(count, start, is_narrow):
            half = count // 2
            there_and_here(b, 0, rows_of(b, left, start, count), at_right).wait_recv()
            there_and_here(b, 2, rows_of(b, left, start, half), at_right).start()
            onward(b, left, 0, start, count, is_narrow)
            there_and_here(b, 1, rows_of(b, right, start, count), at_left).wait_recv()
            there_and_here(b, 3, rows_of(b, right, start + half, half), at_left).start()
            onward(b, right, 1, start, count, is_narrow)

        both(b, do)

    def stage2(b):
        def do(count, start, is_narrow):
            half = count // 2
            there_and_here(b, 2, rows_of(b, far, start, half), at_right).wait_recv()
            there_and_here(b, 3, rows_of(b, far, start + half, half), at_left).wait_recv()
            onward(b, far, 2, start, count, is_narrow)

        both(b, do)

    def stage3(b):
        @pl.when(jnp.logical_not(narrow(b)))
        def _():
            count, start = part // 4, (2 * (1 - pair) + core) * (part // 4)
            for k, origin in enumerate(origins):
                ref = rows_of(b, origin, start, count)
                there_and_here(b, 4 + k, ref, at_pair).wait_recv()
                there_and_here(b, 10 + k, ref, at_core).start()

    def arrived(b):
        def do(count, _, is_narrow):
            for k, origin in enumerate(origins):
                there_and_here(b, 7 + k, rows_of(b, origin, 0, count), at_core).wait_recv()
                if not is_narrow:
                    there_and_here(b, 10 + k, rows_of(b, origin, 0, count), at_core).wait_recv()

        both(b, do)

    def sent(b):
        def do(count, _, is_narrow):
            half = count // 2
            for i, size in ((0, count), (1, count), (2, half), (3, half)):
                there_and_here(b, i, rows_of(b, me, 0, size), at_right).wait_send()
            for i in (7, 8, 9) if is_narrow else range(4, 13):
                there_and_here(b, i, rows_of(b, me, 0, count), at_core).wait_send()

        both(b, do)

    def kv_copy(h, i, ref, there):
        return pltpu.make_async_remote_copy(src_ref=ref, dst_ref=ref, send_sem=kv_send.at[h, i], recv_sem=kv_recv.at[h, i],
                                            device_id=there, device_id_type=MESH)

    def kv_at(h, origin, which=None):
        span = pl.ds(pl.multiple_of(origin * rows, 128), rows)
        return kv_s.at[h, :, span, :] if which is None else kv_s.at[h, which, span, :]

    def kv_stage0(h):
        kv_copy(h, 0, kv_at(h, me), at_right).start()
        kv_copy(h, 1, kv_at(h, me), at_left).start()

    def kv_stage1(h):
        kv_copy(h, 0, kv_at(h, left), at_right).wait_recv()
        kv_copy(h, 2, kv_at(h, left, 0), at_right).start()
        kv_copy(h, 1, kv_at(h, right), at_left).wait_recv()
        kv_copy(h, 3, kv_at(h, right, 1), at_left).start()

    def kv_arrived(h):
        kv_copy(h, 2, kv_at(h, far, 0), at_right).wait_recv()
        kv_copy(h, 3, kv_at(h, far, 1), at_left).wait_recv()

    def kv_sent(h):
        for i in range(2):
            kv_copy(h, i, kv_at(h, me), at_right).wait_send()
        for i in range(2):
            kv_copy(h, 2 + i, kv_at(h, me, 0), at_right).wait_send()

    KV0 = 4
    last = blocks + 2

    def tick(k, _=None):
        pl.when((k >= 2) & (k - 2 < blocks))(lambda: stage3(k - 2))
        pl.when((k >= 1) & (k - 1 < blocks))(lambda: stage2(k - 1))
        pl.when(k < blocks)(lambda: stage1(k))
        h = lax.div(k - KV0, 2)
        pl.when((k >= KV0) & (h < kvh) & (lax.rem(k - KV0, 2) == 1))(lambda: kv_stage1(h))
        pl.when((k >= KV0) & (h < kvh) & (lax.rem(k - KV0, 2) == 0))(lambda: kv_stage0(h))
        pl.when(k + AHEAD < blocks)(lambda: stage0(k + AHEAD))

    def turn(k):
        pl.when(k < last)(lambda: tick(k))
        return jnp.minimum(k + 1, last)

    def until(k, target):
        target = jnp.minimum(target, last)
        lax.fori_loop(k, target, lambda i, _: tick(i), None)
        return jnp.maximum(k, target)

    def loads(b, slot, src, col, do):
        for o in range(n):
            into = w_s.at[slot, pl.ds(o * part, part), :]

            @pl.when(me == o)
            def _():
                own = src.at[:, pl.ds(pl.multiple_of(col * TILE, TILE), TILE)]
                do(pltpu.make_async_copy(own, into, load_sem.at[slot, o]))

            @pl.when(me != o)
            def _():
                do(pltpu.make_async_copy(full_ref.at[b, pl.ds(o * part, part), :], into, load_sem.at[slot, o]))

    def load(b, slot, src, col):
        arrived(b)
        loads(b, slot, src, col, lambda c: c.start())

    def loaded(b, slot, src, col):
        loads(b, slot, src, col, lambda c: c.wait())

    for b in range(AHEAD):
        stage0(b)
    gap_s[...] = lax.broadcasted_iota(jnp.int32, gap_s.shape, 1) - lax.broadcasted_iota(jnp.int32, gap_s.shape, 0)
    x_in.wait()

    @pl.loop(0, rows // 64)
    def _(i):
        at = pl.ds(pl.multiple_of(i * 64, 64), 64)
        wide = o_s[at, :].astype(jnp.float32)
        scale = lax.rsqrt(jnp.mean(wide * wide, -1, keepdims=True) + 1e-6)
        a_s[at, :] = (wide * scale * gain_ref[...].astype(jnp.float32)).astype(jnp.bfloat16)

    def chunks(body):
        @pl.loop(0, rows // CHUNK)
        def _(m):
            body(pl.multiple_of(m * CHUNK, CHUNK))

    def turned(t, at):
        cos, sin = cos_ref[pl.ds(at, CHUNK), :], sin_ref[pl.ds(at, CHUNK), :]
        out = []
        for i in range(TILE // HEAD):
            w = t[:, i * HEAD : (i + 1) * HEAD].astype(jnp.float32)
            out.append((w * cos + pltpu.roll(w, HEAD // 2, 1) * sin).astype(jnp.bfloat16))
        return out

    k_now = until(0, 3)
    load(0, 0, wk_ref, 0)
    k_now = until(k_now, 4)
    load(1, 1, wv_ref, 0)
    loaded(0, 0, wk_ref, 0)

    def keys(at):
        t = _dot(a_s[pl.ds(at, CHUNK), :], w_s[0], 1, 0).astype(jnp.bfloat16)
        for i, head in enumerate(turned(t, at)):
            kv_s[i, 0, pl.ds(pl.multiple_of(me * rows + at, CHUNK), CHUNK), :] = head

    chunks(keys)
    loaded(1, 1, wv_ref, 0)

    def values(at):
        t = _dot(a_s[pl.ds(at, CHUNK), :], w_s[1], 1, 0).astype(jnp.bfloat16)
        for i in range(kvh):
            kv_s[i, 1, pl.ds(pl.multiple_of(me * rows + at, CHUNK), CHUNK), :] = t[:, i * HEAD : (i + 1) * HEAD]

    chunks(values)

    per = nq // kvh
    heads = TILE // HEAD
    e = HEAD**-0.5 * LOG2E
    k_now = until(k_now, 5)
    load(2, 0, wq_ref, 0)

    def attend(h, iq, k_now):
        at_q = pl.ds(pl.multiple_of(iq * BQ, BQ), BQ)
        for i in range(g):
            top_s[i : i + 1, :] = jnp.full((1, BQ), NEG, jnp.float32)
            mix_s[i] = jnp.zeros((HEAD + 8, BQ), jnp.float32)
        ones = jnp.ones((8, BK), jnp.bfloat16)

        def block(j, masked):
            at_k = pl.ds(pl.multiple_of(j * BK, BK), BK)
            k = kv_s[h, 0, at_k, :]
            v = jnp.concatenate([kv_s[h, 1, at_k, :].T, ones], axis=0)
            scores = [_dot(k, q_s[at_q, i * HEAD : (i + 1) * HEAD], 1, 1) for i in range(g)]
            weights, keeps = [], []
            for i, s in enumerate(scores):
                if masked:
                    s = jnp.where(gap_s[...] >= 0, s, HIDDEN)
                old = top_s[i : i + 1, :]
                top = jnp.maximum(old, s.max(axis=0, keepdims=True))
                top_s[i : i + 1, :] = top
                weights.append(jnp.exp2((s - top) * e).astype(jnp.bfloat16))
                keeps.append(jnp.exp2((old - top) * e))
            for i, (p, keep) in enumerate(zip(weights, keeps)):
                mix_s[i] = mix_s[i] * keep + _dot(v, p, 1, 0)

        whole = lax.div(me * rows, BK) + iq

        def segment(i, k_now):
            lax.fori_loop(i * SEG, jnp.minimum((i + 1) * SEG, whole), lambda j, _: block(j, False), None)
            return turn(k_now)

        k_now = lax.fori_loop(0, lax.div(whole + SEG - 1, SEG), segment, k_now)
        block(whole, True)
        for i in range(g):
            total = mix_s[i, HEAD : HEAD + 1, :]
            out = (mix_s[i, :HEAD, :] * (1 / total)).T.astype(jnp.bfloat16)
            o_s[at_q, pl.ds(pl.multiple_of(h * g * HEAD + i * HEAD, HEAD), HEAD)] = out
        return k_now

    def key_head(h, k_now):
        for t in range(per):
            b = 2 + per * h + t
            if t + 1 < per:
                k_now = until(k_now, b + 1 + 3)
                load(b + 1, (t + 1) % 2, wq_ref, b - 1)
            loaded(b, t % 2, wq_ref, b - 2)

            def queries(at):
                out = turned(_dot(a_s[pl.ds(at, CHUNK), :], w_s[t % 2], 1, 0).astype(jnp.bfloat16), at)
                for i in range(heads):
                    q_s[pl.ds(at, CHUNK), (t * heads + i) * HEAD : (t * heads + i + 1) * HEAD] = out[i]

            chunks(queries)
        k_now = until(k_now, KV0 + 2 * h + 2)
        kv_arrived(h)
        steps = rows // BQ
        k_now = lax.fori_loop(0, steps - 1, lambda iq, k: attend(h, iq, k), k_now)
        b = 2 + per * (h + 1)
        k_now = until(k_now, b + 3)

        @pl.when(h + 1 < kvh)
        def _():
            load(b, 0, wq_ref, b - 2)

        @pl.when(h + 1 == kvh)
        def _():
            load(b, 0, wo_ref, 0)

        return attend(h, steps - 1, k_now)

    k_now = lax.fori_loop(0, kvh, key_head, k_now)

    def x_tile(t, slot):
        return pltpu.make_async_copy(x_ref.at[:, pl.ds(pl.multiple_of(t * TILE, TILE), TILE)], xt_s.at[slot], x_sem.at[slot])

    def y_tile(t, slot):
        return pltpu.make_async_copy(yt_s.at[slot], y_ref.at[:, pl.ds(pl.multiple_of(t * TILE, TILE), TILE)], y_sem.at[slot])

    x_tile(0, 0).start()

    def project(t, k_now):
        slot, b = lax.rem(t, 2), 2 + nq + t
        other = 1 - slot
        k_now = until(k_now, b + 1 + 3)

        @pl.when(t + 1 < no)
        def _():
            load(b + 1, other, wo_ref, t + 1)
            x_tile(t + 1, other).start()

        loaded(b, slot, wo_ref, t)
        x_tile(t, slot).wait()
        pl.when(t >= 2)(lambda: y_tile(t - 2, slot).wait())

        def outputs(at):
            y = _dot(o_s[pl.ds(at, CHUNK), :], w_s[slot], 1, 0)
            yt_s[slot, pl.ds(at, CHUNK), :] = (xt_s[slot, pl.ds(at, CHUNK), :].astype(jnp.float32) + y).astype(jnp.bfloat16)

        chunks(outputs)
        y_tile(t, slot).start()
        return k_now

    lax.fori_loop(0, no, project, k_now)
    for t in range(max(no - 2, 0), no):
        y_tile(t, t % 2).wait()
    lax.fori_loop(0, blocks, lambda b, _: sent(b), None)
    lax.fori_loop(0, kvh, lambda h, _: kv_sent(h), None)


def solution(mesh):
    n = mesh.shape["sp"]

    def step(x, gain, wq, wk, wv, wo):
        rows, width = x.shape
        part = wq.shape[0]
        kvh = wk.shape[1] // HEAD
        g = wq.shape[1] // wk.shape[1]
        nq, no = wq.shape[1] // TILE, wo.shape[1] // TILE
        blocks = 2 + nq + no
        half = HEAD // 2
        place = lax.axis_index("sp") * rows + jnp.arange(rows)
        angle = place.astype(jnp.float32)[:, None] * THETA ** (-jnp.arange(half, dtype=jnp.float32) / half)
        cos, sin = jnp.cos(angle), jnp.sin(angle)
        cos, sin = jnp.concatenate([cos, cos], 1), jnp.concatenate([-sin, sin], 1)
        bf, f32 = jnp.bfloat16, jnp.float32
        hbm, vmem = pl.BlockSpec(memory_space=pl.ANY), pl.BlockSpec(memory_space=pltpu.VMEM)
        dma = pltpu.SemaphoreType.DMA
        y, _ = pl.pallas_call(
            functools.partial(_kernel, n, nq, no, g),
            out_shape=[jax.ShapeDtypeStruct((rows, width), bf), jax.ShapeDtypeStruct((blocks, n * part, TILE), bf)],
            in_specs=[hbm, vmem, vmem, vmem, hbm, hbm, hbm, hbm],
            out_specs=[hbm, hbm],
            scratch_shapes=[
                pltpu.VMEM((rows, width), bf),
                pltpu.VMEM((rows, width), bf),
                pltpu.VMEM((kvh, 2, n * rows, HEAD), bf),
                pltpu.VMEM((2, n * part, TILE), bf),
                pltpu.VMEM((rows, g * HEAD), bf),
                pltpu.VMEM((g, HEAD + 8, BQ), f32),
                pltpu.VMEM((g, BQ), f32),
                pltpu.VMEM((BK, BQ), jnp.int32),
                pltpu.VMEM((2, rows, TILE), bf),
                pltpu.VMEM((2, rows, TILE), bf),
                dma((blocks, 13)),
                dma((blocks, 13)),
                dma((kvh, 4)),
                dma((kvh, 4)),
                dma((2, n)),
                dma((2,)),
                dma((2,)),
                dma,
            ],
            compiler_params=pltpu.CompilerParams(collective_id=0, has_side_effects=True, vmem_limit_bytes=63 * 2**20),
        )(x, gain[None], cos, sin, wq, wk, wv, wo)
        return y

    tokens, whole = P(("dp", "sp"), None), P("sp", None)
    return jax.shard_map(
        step,
        mesh=mesh,
        in_specs=(tokens, P(None), whole, whole, whole, whole),
        out_specs=tokens,
        check_vma=False,
    )
```

```python
import functools

import jax
import jax.numpy as jnp
from jax import lax
from jax.experimental import pallas as pl
from jax.experimental.pallas import tpu as pltpu
from jax.sharding import PartitionSpec as P

HEAD = 128
THETA = 10000
NEG = -1e30
HIDDEN = 2 * NEG
LOG2E = 1.4426950408889634
TILE = 512
CHUNK = 1024
BQ = 512
BK = 512
SEG = 8
MESH = pl.DeviceIdType.MESH
FLAGS = {}
ORDER = 0
AHEAD = 2
MORE = 0
TURN = 0
RING_BUSY = 9
RING_FREE = 10.5


def _dot(a, b, ca, cb):
    return lax.dot_general(a, b, (((ca,), (cb,)), ((), ())), preferred_element_type=jnp.float32)


def _kernel(n, nq, no, g, x_ref, gain_ref, cos_ref, sin_ref, wq_ref, wk_ref, wv_ref, wo_ref, y_ref, full_ref,
            a_s, o_s, kv_s, w_s, q_s, mix_s, top_s, gap_s, xt_s, yt_s,
            send, recv, kv_send, kv_recv, load_sem, x_sem, y_sem, in_sem):
    me, dp = lax.axis_index("sp"), lax.axis_index("dp")
    rows = x_ref.shape[0]
    part = wq_ref.shape[0]
    kvh = kv_s.shape[0]
    blocks = 2 + nq + no
    right, left, far = lax.rem(me + 1, n), lax.rem(me + n - 1, n), lax.rem(me + 2, n)
    core, pair = lax.rem(dp, 2), lax.rem(lax.div(dp, 2), 2)
    at_right, at_left = {"sp": right}, {"sp": left}
    at_core, at_pair = {"dp": dp + 1 - 2 * core}, {"dp": dp + 2 - 4 * pair}
    origins = (left, right, far)

    barrier = pltpu.get_barrier_semaphore()
    for there in (at_right, at_left, at_core, at_pair):
        pl.semaphore_signal(barrier, inc=1, device_id=there, device_id_type=MESH)
    x_in = pltpu.make_async_copy(x_ref, o_s, in_sem)
    x_in.start()
    pl.semaphore_wait(barrier, 4)

    base, half_part = core * (part // 2), part // 2

    def modes(b):
        busy = (b >= 4) & (b < 2 + nq + 3)
        narrow = b == blocks - 1
        return ((busy, int(RING_BUSY * half_part) // 16), (narrow, half_part),
                (jnp.logical_not(busy | narrow), int(RING_FREE * half_part) // 16))

    def copy(b, i, src, dst, there):
        return pltpu.make_async_remote_copy(src_ref=src, dst_ref=dst, send_sem=send.at[b, i], recv_sem=recv.at[b, i],
                                            device_id=there, device_id_type=MESH)

    def there_and_here(b, i, ref, there):
        return copy(b, i, ref, ref, there)

    def rows_of(b, origin, start, count):
        return full_ref.at[b, pl.ds(pl.multiple_of(origin * part + start, 8), count), :]

    def both(b, do):
        for when, count in modes(b):
            @pl.when(when)
            def _():
                theirs = half_part - count
                do(count, base + pair * theirs, theirs)

    def stage0(b):
        def do(count, start, theirs):
            def go(src, col):
                own = src.at[pl.ds(pl.multiple_of(start, 8), count), pl.ds(pl.multiple_of(col * TILE, TILE), TILE)]
                copy(b, 0, own, rows_of(b, me, start, count), at_right).start()
                copy(b, 1, own, rows_of(b, me, start, count), at_left).start()

            pl.when(b == 0)(lambda: go(wk_ref, 0))
            pl.when(b == 1)(lambda: go(wv_ref, 0))
            pl.when((b >= 2) & (b < 2 + nq))(lambda: go(wq_ref, b - 2))
            pl.when(b >= 2 + nq)(lambda: go(wo_ref, b - 2 - nq))

        both(b, do)

    def onward(b, k, start, count, theirs):
        if theirs:
            there_and_here(b, 4 + k, rows_of(b, origins[k], base + pair * count, theirs), at_pair).start()
        there_and_here(b, 7 + k, rows_of(b, origins[k], start, count), at_core).start()

    def stage1(b):
        def do(count, start, theirs):
            half = count // 2
            there_and_here(b, 0, rows_of(b, left, start, count), at_right).wait_recv()
            there_and_here(b, 2, rows_of(b, left, start, half), at_right).start()
            onward(b, 0, start, count, theirs)
            there_and_here(b, 1, rows_of(b, right, start, count), at_left).wait_recv()
            there_and_here(b, 3, rows_of(b, right, start + half, half), at_left).start()
            onward(b, 1, start, count, theirs)

        both(b, do)

    def stage2(b):
        def do(count, start, theirs):
            half = count // 2
            there_and_here(b, 2, rows_of(b, far, start, half), at_right).wait_recv()
            there_and_here(b, 3, rows_of(b, far, start + half, half), at_left).wait_recv()
            onward(b, 2, start, count, theirs)

        both(b, do)

    def stage3(b):
        def do(count, start, theirs):
            if theirs:
                for k, origin in enumerate(origins):
                    ref = rows_of(b, origin, base + (1 - pair) * count, theirs)
                    there_and_here(b, 4 + k, ref, at_pair).wait_recv()
                    there_and_here(b, 10 + k, ref, at_core).start()

        both(b, do)

    def arrived(b):
        def do(count, _, theirs):
            for k, origin in enumerate(origins):
                there_and_here(b, 7 + k, rows_of(b, origin, 0, count), at_core).wait_recv()
                if theirs:
                    there_and_here(b, 10 + k, rows_of(b, origin, 0, theirs), at_core).wait_recv()

        both(b, do)

    def sent(b):
        def do(count, _, theirs):
            half = count // 2
            sizes = {0: count, 1: count, 2: half, 3: half, 7: count, 8: count, 9: count}
            if theirs:
                sizes |= {4: theirs, 5: theirs, 6: theirs, 10: theirs, 11: theirs, 12: theirs}
            for i, size in sizes.items():
                there_and_here(b, i, rows_of(b, me, 0, size), at_right).wait_send()

        both(b, do)

    def kv_copy(h, i, ref, there):
        return pltpu.make_async_remote_copy(src_ref=ref, dst_ref=ref, send_sem=kv_send.at[h, i], recv_sem=kv_recv.at[h, i],
                                            device_id=there, device_id_type=MESH)

    def kv_at(h, origin, which=None):
        span = pl.ds(pl.multiple_of(origin * rows, 128), rows)
        return kv_s.at[h, :, span, :] if which is None else kv_s.at[h, which, span, :]

    def kv_stage0(h):
        kv_copy(h, 0, kv_at(h, me), at_right).start()
        kv_copy(h, 1, kv_at(h, me), at_left).start()

    def kv_stage1(h):
        kv_copy(h, 0, kv_at(h, left), at_right).wait_recv()
        kv_copy(h, 2, kv_at(h, left, 0), at_right).start()
        kv_copy(h, 1, kv_at(h, right), at_left).wait_recv()
        kv_copy(h, 3, kv_at(h, right, 1), at_left).start()

    def kv_arrived(h):
        kv_copy(h, 2, kv_at(h, far, 0), at_right).wait_recv()
        kv_copy(h, 3, kv_at(h, far, 1), at_left).wait_recv()

    def kv_sent(h):
        for i in range(2):
            kv_copy(h, i, kv_at(h, me), at_right).wait_send()
        for i in range(2):
            kv_copy(h, 2 + i, kv_at(h, me, 0), at_right).wait_send()

    EVERY = 3
    FIRST = 4
    last = blocks + 2

    def tick(k):
        pl.when((k - 2 >= FIRST) & (k - 2 < blocks))(lambda: stage3(k - 2))
        pl.when((k - 1 >= FIRST) & (k - 1 < blocks))(lambda: stage2(k - 1))
        pl.when(k < blocks)(lambda: stage1(k))
        h, at = lax.div(k - FIRST, EVERY) + 1, lax.rem(k - FIRST, EVERY)
        pl.when((h < kvh) & (at == 1))(lambda: kv_stage1(h))
        pl.when((h < kvh) & (at == 0))(lambda: kv_stage0(h))
        b = k + AHEAD + jnp.clip(k - FIRST, 0, MORE)
        pl.when(b < blocks)(lambda: stage0(b))
        pl.when((k < FIRST + MORE) & (b + 1 < blocks))(lambda: stage0(b + 1))

    def complete(b):
        return jnp.where(b < FIRST, 0, b + 3)

    def turn(k):
        pl.when(k < last)(lambda: tick(k))
        return jnp.minimum(k + 1, last)

    def until(k, target):
        target = jnp.minimum(target, last)
        lax.fori_loop(k, target, lambda i, _: tick(i), None)
        return jnp.maximum(k, target)

    def loads(b, slot, src, col, do):
        for o in range(n):
            into = w_s.at[slot, pl.ds(o * part, part), :]

            @pl.when(me == o)
            def _():
                own = src.at[:, pl.ds(pl.multiple_of(col * TILE, TILE), TILE)]
                do(pltpu.make_async_copy(own, into, load_sem.at[slot, o]))

            @pl.when(me != o)
            def _():
                do(pltpu.make_async_copy(full_ref.at[b, pl.ds(o * part, part), :], into, load_sem.at[slot, o]))

    def load(b, slot, src, col):
        arrived(b)
        loads(b, slot, src, col, lambda c: c.start())

    def loaded(b, slot, src, col):
        loads(b, slot, src, col, lambda c: c.wait())

    for b in range(AHEAD):
        stage0(b)
    gap_s[...] = lax.broadcasted_iota(jnp.int32, gap_s.shape, 1) - lax.broadcasted_iota(jnp.int32, gap_s.shape, 0)
    x_in.wait()

    @pl.loop(0, rows // 64)
    def _(i):
        at = pl.ds(pl.multiple_of(i * 64, 64), 64)
        wide = o_s[at, :].astype(jnp.float32)
        scale = lax.rsqrt(jnp.mean(wide * wide, -1, keepdims=True) + 1e-6)
        a_s[at, :] = (wide * scale * gain_ref[...].astype(jnp.float32)[None]).astype(jnp.bfloat16)

    def chunks(body):
        @pl.loop(0, rows // CHUNK)
        def _(m):
            body(pl.multiple_of(m * CHUNK, CHUNK))

    def turned(t, at):
        cos, sin = cos_ref[pl.ds(at, CHUNK), :], sin_ref[pl.ds(at, CHUNK), :]
        out = []
        for i in range(TILE // HEAD):
            w = t[:, i * HEAD : (i + 1) * HEAD].astype(jnp.float32)
            out.append((w * cos + pltpu.roll(w, HEAD // 2, 1) * sin).astype(jnp.bfloat16))
        return out

    def keys(at):
        t = _dot(a_s[pl.ds(at, CHUNK), :], w_s[0], 1, 0).astype(jnp.bfloat16)
        for i, head in enumerate(turned(t, at)):
            kv_s[i, 0, pl.ds(pl.multiple_of(me * rows + at, CHUNK), CHUNK), :] = head

    def values(at):
        t = _dot(a_s[pl.ds(at, CHUNK), :], w_s[1], 1, 0).astype(jnp.bfloat16)
        for i in range(kvh):
            kv_s[i, 1, pl.ds(pl.multiple_of(me * rows + at, CHUNK), CHUNK), :] = t[:, i * HEAD : (i + 1) * HEAD]

    stage1(0)
    stage0(2)
    stage2(0)
    stage1(1)
    stage0(3)
    stage3(0)
    load(0, 0, wk_ref, 0)
    stage2(1)
    loaded(0, 0, wk_ref, 0)
    chunks(keys)
    stage3(1)
    load(1, 1, wv_ref, 0)
    stage1(2)
    loaded(1, 1, wv_ref, 0)
    chunks(values)
    kv_stage0(0)
    stage2(2)
    stage1(3)
    stage3(2)
    load(2, 0, wq_ref, 0)
    kv_stage1(0)
    stage0(4)
    stage2(3)
    stage0(5)
    stage3(3)
    k_now = jnp.int32(FIRST)

    per = nq // kvh
    heads = TILE // HEAD
    e = HEAD**-0.5 * LOG2E

    def attend(h, iq, k_now):
        at_q = pl.ds(pl.multiple_of(iq * BQ, BQ), BQ)
        for i in range(g):
            top_s[i : i + 1, :] = jnp.full((1, BQ), NEG, jnp.float32)
            mix_s[i] = jnp.zeros((HEAD + 8, BQ), jnp.float32)
        ones = jnp.ones((8, BK), jnp.bfloat16)

        def block(j, masked):
            at_k = pl.ds(pl.multiple_of(j * BK, BK), BK)
            k = kv_s[h, 0, at_k, :]
            v = jnp.concatenate([kv_s[h, 1, at_k, :].T, ones], axis=0)
            def score(i):
                return _dot(k, q_s[at_q, i * HEAD : (i + 1) * HEAD], 1, 1)

            def weigh(i, s):
                if masked:
                    s = jnp.where(gap_s[...] >= 0, s, HIDDEN)
                old = top_s[i : i + 1, :]
                top = jnp.maximum(old, s.max(axis=0, keepdims=True))
                top_s[i : i + 1, :] = top
                return jnp.exp2((s - top) * e).astype(jnp.bfloat16), jnp.exp2((old - top) * e)

            def mix(i, p, keep):
                mix_s[i] = mix_s[i] * keep + _dot(v, p, 1, 0)

            if ORDER == 0:
                scores = [score(i) for i in range(g)]
                both = [weigh(i, s) for i, s in enumerate(scores)]
                for i in range(g):
                    mix(i, *both[i])
            else:
                scores = {i: score(i) for i in range(ORDER)}
                held = None
                for i in range(g):
                    if i + ORDER < g:
                        scores[i + ORDER] = score(i + ORDER)
                    now = weigh(i, scores.pop(i))
                    if held:
                        mix(i - 1, *held)
                    held = now
                mix(g - 1, *held)

        whole = lax.div(me * rows, BK) + iq

        def segment(i, k_now):
            lax.fori_loop(i * SEG, jnp.minimum((i + 1) * SEG, whole), lambda j, _: block(j, False), None)
            return turn(k_now)

        k_now = lax.fori_loop(0, lax.div(whole + SEG - 1, SEG), segment, k_now)
        block(whole, True)
        for i in range(g):
            total = mix_s[i, HEAD : HEAD + 1, :]
            out = (mix_s[i, :HEAD, :] * (1 / total)).T.astype(jnp.bfloat16)
            o_s[at_q, pl.ds(pl.multiple_of(h * g * HEAD + i * HEAD, HEAD), HEAD)] = out
        return k_now

    def key_head(h, k_now):
        for t in range(per):
            b = 2 + per * h + t
            if t + 1 < per:
                k_now = until(k_now, complete(b + 1))
                load(b + 1, (t + 1) % 2, wq_ref, b - 1)
            loaded(b, t % 2, wq_ref, b - 2)

            def queries(at):
                out = turned(_dot(a_s[pl.ds(at, CHUNK), :], w_s[t % 2], 1, 0).astype(jnp.bfloat16), at)
                for i in range(heads):
                    q_s[pl.ds(at, CHUNK), (t * heads + i) * HEAD : (t * heads + i + 1) * HEAD] = out[i]

            chunks(queries)
        k_now = lax.cond(h >= TURN, turn, lambda k: k, k_now)
        k_now = until(k_now, jnp.where(h == 0, 0, FIRST + EVERY * (h - 1) + 2))
        kv_arrived(h)
        steps = rows // BQ
        k_now = lax.fori_loop(0, steps - 1, lambda iq, k: attend(h, iq, k), k_now)
        b = 2 + per * (h + 1)
        k_now = until(k_now, complete(b))

        @pl.when(h + 1 < kvh)
        def _():
            load(b, 0, wq_ref, b - 2)

        @pl.when(h + 1 == kvh)
        def _():
            load(b, 0, wo_ref, 0)

        return attend(h, steps - 1, k_now)

    k_now = lax.fori_loop(0, kvh, key_head, k_now)

    def x_tile(t, slot):
        return pltpu.make_async_copy(x_ref.at[:, pl.ds(pl.multiple_of(t * TILE, TILE), TILE)], xt_s.at[slot], x_sem.at[slot])

    def y_tile(t, slot):
        return pltpu.make_async_copy(yt_s.at[slot], y_ref.at[:, pl.ds(pl.multiple_of(t * TILE, TILE), TILE)], y_sem.at[slot])

    x_tile(0, 0).start()

    def project(t, k_now):
        slot, b = lax.rem(t, 2), 2 + nq + t
        other = 1 - slot
        k_now = until(k_now, complete(b + 1))

        @pl.when(t + 1 < no)
        def _():
            load(b + 1, other, wo_ref, t + 1)
            x_tile(t + 1, other).start()

        loaded(b, slot, wo_ref, t)
        x_tile(t, slot).wait()
        pl.when(t >= 2)(lambda: y_tile(t - 2, slot).wait())

        def outputs(at):
            y = _dot(o_s[pl.ds(at, CHUNK), :], w_s[slot], 1, 0)
            yt_s[slot, pl.ds(at, CHUNK), :] = (xt_s[slot, pl.ds(at, CHUNK), :].astype(jnp.float32) + y).astype(jnp.bfloat16)

        chunks(outputs)
        y_tile(t, slot).start()
        return k_now

    lax.fori_loop(0, no, project, k_now)
    for t in range(max(no - 2, 0), no):
        y_tile(t, t % 2).wait()
    lax.fori_loop(0, blocks, lambda b, _: sent(b), None)
    lax.fori_loop(0, kvh, lambda h, _: kv_sent(h), None)


def solution(mesh):
    n = mesh.shape["sp"]

    def step(x, gain, wq, wk, wv, wo):
        rows, width = x.shape
        part = wq.shape[0]
        kvh = wk.shape[1] // HEAD
        g = wq.shape[1] // wk.shape[1]
        nq, no = wq.shape[1] // TILE, wo.shape[1] // TILE
        blocks = 2 + nq + no
        half = HEAD // 2
        place = lax.axis_index("sp") * rows + jnp.arange(rows)
        lane = jnp.arange(HEAD)
        angle = place.astype(jnp.float32)[:, None] * THETA ** (-(lane % half).astype(jnp.float32) / half)
        cos, sin = jnp.cos(angle), jnp.where(lane < half, -1.0, 1.0) * jnp.sin(angle)
        bf, f32 = jnp.bfloat16, jnp.float32
        hbm, vmem = pl.BlockSpec(memory_space=pl.ANY), pl.BlockSpec(memory_space=pltpu.VMEM)
        dma = pltpu.SemaphoreType.DMA
        y, _ = pl.pallas_call(
            functools.partial(_kernel, n, nq, no, g),
            out_shape=[jax.ShapeDtypeStruct((rows, width), bf), jax.ShapeDtypeStruct((blocks, n * part, TILE), bf)],
            in_specs=[hbm, vmem, vmem, vmem, hbm, hbm, hbm, hbm],
            out_specs=[hbm, hbm],
            scratch_shapes=[
                pltpu.VMEM((rows, width), bf),
                pltpu.VMEM((rows, width), bf),
                pltpu.VMEM((kvh, 2, n * rows, HEAD), bf),
                pltpu.VMEM((2, n * part, TILE), bf),
                pltpu.VMEM((rows, g * HEAD), bf),
                pltpu.VMEM((g, HEAD + 8, BQ), f32),
                pltpu.VMEM((g, BQ), f32),
                pltpu.VMEM((BK, BQ), jnp.int32),
                pltpu.VMEM((2, rows, TILE), bf),
                pltpu.VMEM((2, rows, TILE), bf),
                dma((blocks, 13)),
                dma((blocks, 13)),
                dma((kvh, 4)),
                dma((kvh, 4)),
                dma((2, n)),
                dma((2,)),
                dma((2,)),
                dma,
            ],
            compiler_params=pltpu.CompilerParams(collective_id=0, has_side_effects=True, vmem_limit_bytes=63 * 2**20, flags=FLAGS),
        )(x, gain, cos, sin, wq, wk, wv, wo)
        return y

    tokens, whole = P(("dp", "sp"), None), P("sp", None)
    return jax.shard_map(
        step,
        mesh=mesh,
        in_specs=(tokens, P(None), whole, whole, whole, whole),
        out_specs=tokens,
        check_vma=False,
    )
```

```python
import functools

import jax
import jax.numpy as jnp
from jax import lax
from jax.experimental import pallas as pl
from jax.experimental.pallas import tpu as pltpu
from jax.sharding import PartitionSpec as P

HEAD = 128
THETA = 10000
NEG = -1e30
HIDDEN = 2 * NEG
LOG2E = 1.4426950408889634
TILE = 512
CHUNK = 1024
SMALL = 256
BQ = 512
BK = 512
SEG = 8
MESH = pl.DeviceIdType.MESH
FLAGS = {}
AHEAD = 2
EVERY = 3
RING_BUSY = 8.5
RING_FREE = 10


def _dot(a, b, ca, cb):
    return lax.dot_general(a, b, (((ca,), (cb,)), ((), ())), preferred_element_type=jnp.float32)


def _kernel(n, nq, no, g, x_ref, gain_ref, cos_ref, sin_ref, wq_ref, wk_ref, wv_ref, wo_ref, y_ref, full_ref,
            a_s, o_s, kv_s, w_s, q_s, mix_s, top_s, gap_s, xt_s, yt_s,
            send, recv, kv_send, kv_recv, load_sem, x_sem, y_sem, in_sem):
    me, dp = lax.axis_index("sp"), lax.axis_index("dp")
    rows = x_ref.shape[0]
    part = wq_ref.shape[0]
    kvh = kv_s.shape[0]
    blocks = 2 + nq + no
    right, left, far = lax.rem(me + 1, n), lax.rem(me + n - 1, n), lax.rem(me + 2, n)
    core, pair = lax.rem(dp, 2), lax.rem(lax.div(dp, 2), 2)
    at_right, at_left = {"sp": right}, {"sp": left}
    at_core, at_pair = {"dp": dp + 1 - 2 * core}, {"dp": dp + 2 - 4 * pair}
    origins = (left, right, far)

    barrier = pltpu.get_barrier_semaphore()
    for there in (at_right, at_left, at_core, at_pair):
        pl.semaphore_signal(barrier, inc=1, device_id=there, device_id_type=MESH)
    x_in = pltpu.make_async_copy(x_ref, o_s, in_sem)
    x_in.start()
    pl.semaphore_wait(barrier, 4)

    base, half_part = core * (part // 2), part // 2

    def modes(b):
        busy = (b >= 4) & (b < 2 + nq + 3)
        narrow = b == blocks - 1
        return ((busy, int(RING_BUSY * half_part) // 16), (narrow, half_part),
                (jnp.logical_not(busy | narrow), int(RING_FREE * half_part) // 16))

    def copy(b, i, src, dst, there):
        return pltpu.make_async_remote_copy(src_ref=src, dst_ref=dst, send_sem=send.at[b, i], recv_sem=recv.at[b, i],
                                            device_id=there, device_id_type=MESH)

    def there_and_here(b, i, ref, there):
        return copy(b, i, ref, ref, there)

    def rows_of(b, origin, start, count):
        return full_ref.at[b, pl.ds(pl.multiple_of(origin * part + start, 8), count), :]

    def both(b, do):
        for when, count in modes(b):
            @pl.when(when)
            def _():
                theirs = half_part - count
                do(count, base + pair * theirs, theirs)

    def stage0(b):
        def do(count, start, theirs):
            def go(src, col):
                own = src.at[pl.ds(pl.multiple_of(start, 8), count), pl.ds(pl.multiple_of(col * TILE, TILE), TILE)]
                copy(b, 0, own, rows_of(b, me, start, count), at_right).start()
                copy(b, 1, own, rows_of(b, me, start, count), at_left).start()

            pl.when(b == 0)(lambda: go(wk_ref, 0))
            pl.when(b == 1)(lambda: go(wv_ref, 0))
            pl.when((b >= 2) & (b < 2 + nq))(lambda: go(wq_ref, b - 2))
            pl.when(b >= 2 + nq)(lambda: go(wo_ref, b - 2 - nq))

        both(b, do)

    def onward(b, k, start, count, theirs):
        if theirs:
            there_and_here(b, 4 + k, rows_of(b, origins[k], base + pair * count, theirs), at_pair).start()
        there_and_here(b, 7 + k, rows_of(b, origins[k], start, count), at_core).start()

    def stage1(b):
        def do(count, start, theirs):
            half = count // 2
            there_and_here(b, 0, rows_of(b, left, start, count), at_right).wait_recv()
            there_and_here(b, 2, rows_of(b, left, start, half), at_right).start()
            onward(b, 0, start, count, theirs)
            there_and_here(b, 1, rows_of(b, right, start, count), at_left).wait_recv()
            there_and_here(b, 3, rows_of(b, right, start + half, half), at_left).start()
            onward(b, 1, start, count, theirs)

        both(b, do)

    def stage2(b):
        def do(count, start, theirs):
            half = count // 2
            there_and_here(b, 2, rows_of(b, far, start, half), at_right).wait_recv()
            there_and_here(b, 3, rows_of(b, far, start + half, half), at_left).wait_recv()
            onward(b, 2, start, count, theirs)

        both(b, do)

    def stage3(b):
        def do(count, start, theirs):
            if theirs:
                for k, origin in enumerate(origins):
                    ref = rows_of(b, origin, base + (1 - pair) * count, theirs)
                    there_and_here(b, 4 + k, ref, at_pair).wait_recv()
                    there_and_here(b, 10 + k, ref, at_core).start()

        both(b, do)

    def arrived(b):
        def do(count, _, theirs):
            for k, origin in enumerate(origins):
                there_and_here(b, 7 + k, rows_of(b, origin, 0, count), at_core).wait_recv()
                if theirs:
                    there_and_here(b, 10 + k, rows_of(b, origin, 0, theirs), at_core).wait_recv()

        both(b, do)

    def sent(b):
        def do(count, _, theirs):
            half = count // 2
            sizes = {0: count, 1: count, 2: half, 3: half, 7: count, 8: count, 9: count}
            if theirs:
                sizes |= {4: theirs, 5: theirs, 6: theirs, 10: theirs, 11: theirs, 12: theirs}
            for i, size in sizes.items():
                there_and_here(b, i, rows_of(b, me, 0, size), at_right).wait_send()

        both(b, do)

    def kv_copy(h, i, ref, there):
        return pltpu.make_async_remote_copy(src_ref=ref, dst_ref=ref, send_sem=kv_send.at[h, i], recv_sem=kv_recv.at[h, i],
                                            device_id=there, device_id_type=MESH)

    def kv_at(h, origin, which=None):
        span = pl.ds(pl.multiple_of(origin * rows, 128), rows)
        return kv_s.at[h, :, span, :] if which is None else kv_s.at[h, which, span, :]

    def kv_stage0(h):
        kv_copy(h, 0, kv_at(h, me), at_right).start()
        kv_copy(h, 1, kv_at(h, me), at_left).start()

    def kv_stage1(h):
        kv_copy(h, 0, kv_at(h, left), at_right).wait_recv()
        kv_copy(h, 2, kv_at(h, left, 0), at_right).start()
        kv_copy(h, 1, kv_at(h, right), at_left).wait_recv()
        kv_copy(h, 3, kv_at(h, right, 1), at_left).start()

    def kv_arrived(h):
        kv_copy(h, 2, kv_at(h, far, 0), at_right).wait_recv()
        kv_copy(h, 3, kv_at(h, far, 1), at_left).wait_recv()

    def kv_sent(h):
        for i in range(2):
            kv_copy(h, i, kv_at(h, me), at_right).wait_send()
        for i in range(2):
            kv_copy(h, 2 + i, kv_at(h, me, 0), at_right).wait_send()

    FIRST = 4
    last = blocks + 2

    def tick(k):
        pl.when((k - 2 >= FIRST) & (k - 2 < blocks))(lambda: stage3(k - 2))
        pl.when((k - 1 >= FIRST) & (k - 1 < blocks))(lambda: stage2(k - 1))
        pl.when(k < blocks)(lambda: stage1(k))
        h, at = lax.div(k - FIRST, EVERY) + 1, lax.rem(k - FIRST, EVERY)
        pl.when((h < kvh) & (at == 1))(lambda: kv_stage1(h))
        pl.when((h < kvh) & (at == 0))(lambda: kv_stage0(h))
        pl.when(k + AHEAD < blocks)(lambda: stage0(k + AHEAD))

    def complete(b):
        return jnp.where(b < FIRST, 0, b + 3)

    def turn(k):
        pl.when(k < last)(lambda: tick(k))
        return jnp.minimum(k + 1, last)

    def until(k, target):
        target = jnp.minimum(target, last)
        lax.fori_loop(k, target, lambda i, _: tick(i), None)
        return jnp.maximum(k, target)

    def loads(b, slot, src, col, do):
        for o in range(n):
            into = w_s.at[slot, pl.ds(o * part, part), :]

            @pl.when(me == o)
            def _():
                own = src.at[:, pl.ds(pl.multiple_of(col * TILE, TILE), TILE)]
                do(pltpu.make_async_copy(own, into, load_sem.at[slot, o]))

            @pl.when(me != o)
            def _():
                do(pltpu.make_async_copy(full_ref.at[b, pl.ds(o * part, part), :], into, load_sem.at[slot, o]))

    def load(b, slot, src, col):
        arrived(b)
        loads(b, slot, src, col, lambda c: c.start())

    def loaded(b, slot, src, col):
        loads(b, slot, src, col, lambda c: c.wait())

    for b in range(AHEAD):
        stage0(b)
    gap_s[...] = lax.broadcasted_iota(jnp.int32, gap_s.shape, 1) - lax.broadcasted_iota(jnp.int32, gap_s.shape, 0)
    x_in.wait()

    @pl.loop(0, rows // 64)
    def _(i):
        at = pl.ds(pl.multiple_of(i * 64, 64), 64)
        wide = o_s[at, :].astype(jnp.float32)
        scale = lax.rsqrt(jnp.mean(wide * wide, -1, keepdims=True) + 1e-6)
        a_s[at, :] = (wide * scale * gain_ref[...].astype(jnp.float32)[None]).astype(jnp.bfloat16)

    def chunks(body, size=CHUNK):
        @pl.loop(0, rows // size)
        def _(m):
            body(pl.multiple_of(m * size, size))

    def turned(t, at):
        cos, sin = cos_ref[pl.ds(at, t.shape[0]), :], sin_ref[pl.ds(at, t.shape[0]), :]
        out = []
        for i in range(TILE // HEAD):
            w = t[:, i * HEAD : (i + 1) * HEAD].astype(jnp.float32)
            out.append((w * cos + pltpu.roll(w, HEAD // 2, 1) * sin).astype(jnp.bfloat16))
        return out

    def keys(at):
        t = _dot(a_s[pl.ds(at, SMALL), :], w_s[0], 1, 0).astype(jnp.bfloat16)
        for i, head in enumerate(turned(t, at)):
            kv_s[i, 0, pl.ds(pl.multiple_of(me * rows + at, SMALL), SMALL), :] = head

    def values(at):
        t = _dot(a_s[pl.ds(at, SMALL), :], w_s[1], 1, 0).astype(jnp.bfloat16)
        for i in range(kvh):
            kv_s[i, 1, pl.ds(pl.multiple_of(me * rows + at, SMALL), SMALL), :] = t[:, i * HEAD : (i + 1) * HEAD]

    stage1(0)
    stage0(2)
    stage2(0)
    stage1(1)
    stage0(3)
    stage3(0)
    load(0, 0, wk_ref, 0)
    stage2(1)
    loaded(0, 0, wk_ref, 0)
    chunks(keys, SMALL)
    stage3(1)
    load(1, 1, wv_ref, 0)
    stage1(2)
    loaded(1, 1, wv_ref, 0)
    chunks(values, SMALL)
    kv_stage0(0)
    stage2(2)
    stage1(3)
    stage3(2)
    load(2, 0, wq_ref, 0)
    kv_stage1(0)
    stage0(4)
    stage2(3)
    stage0(5)
    stage3(3)
    k_now = jnp.int32(FIRST)

    per = nq // kvh
    heads = TILE // HEAD
    e = HEAD**-0.5 * LOG2E

    def attend(h, iq, k_now):
        at_q = pl.ds(pl.multiple_of(iq * BQ, BQ), BQ)
        for i in range(g):
            top_s[i : i + 1, :] = jnp.full((1, BQ), NEG, jnp.float32)
            mix_s[i] = jnp.zeros((HEAD + 8, BQ), jnp.float32)
        ones = jnp.ones((8, BK), jnp.bfloat16)

        def block(j, masked):
            at_k = pl.ds(pl.multiple_of(j * BK, BK), BK)
            k = kv_s[h, 0, at_k, :]
            v = jnp.concatenate([kv_s[h, 1, at_k, :].T, ones], axis=0)
            def score(i):
                return _dot(k, q_s[at_q, i * HEAD : (i + 1) * HEAD], 1, 1)

            def weigh(i, s):
                if masked:
                    s = jnp.where(gap_s[...] >= 0, s, HIDDEN)
                old = top_s[i : i + 1, :]
                top = jnp.maximum(old, s.max(axis=0, keepdims=True))
                top_s[i : i + 1, :] = top
                return jnp.exp2((s - top) * e).astype(jnp.bfloat16), jnp.exp2((old - top) * e)

            def mix(i, p, keep):
                mix_s[i] = mix_s[i] * keep + _dot(v, p, 1, 0)

            scores = [score(i) for i in range(g)]
            weights = [weigh(i, s) for i, s in enumerate(scores)]
            for i in range(g):
                mix(i, *weights[i])

        whole = lax.div(me * rows, BK) + iq

        def segment(i, k_now):
            lax.fori_loop(i * SEG, jnp.minimum((i + 1) * SEG, whole), lambda j, _: block(j, False), None)
            return turn(k_now)

        k_now = lax.fori_loop(0, lax.div(whole + SEG - 1, SEG), segment, k_now)
        block(whole, True)
        for i in range(g):
            total = mix_s[i, HEAD : HEAD + 1, :]
            out = (mix_s[i, :HEAD, :] * (1 / total)).T.astype(jnp.bfloat16)
            o_s[at_q, pl.ds(pl.multiple_of(h * g * HEAD + i * HEAD, HEAD), HEAD)] = out
        return k_now

    steps = rows // BQ

    def key_head(h, k_now):
        def query_tile(t, k_now):
            b, slot = 2 + per * h + t, lax.rem(t, 2)
            k_now = until(k_now, jnp.where(t + 1 < per, complete(b + 1), 0))
            pl.when(t + 1 < per)(lambda: load(b + 1, 1 - slot, wq_ref, b - 1))
            loaded(b, slot, wq_ref, b - 2)

            def queries(at):
                out = turned(_dot(a_s[pl.ds(at, CHUNK), :], w_s[slot], 1, 0).astype(jnp.bfloat16), at)
                for i in range(heads):
                    q_s[pl.ds(at, CHUNK), pl.ds(pl.multiple_of((t * heads + i) * HEAD, HEAD), HEAD)] = out[i]

            chunks(queries)
            return k_now

        k_now = lax.fori_loop(0, per, query_tile, k_now)
        k_now = turn(k_now)
        k_now = until(k_now, jnp.where(h == 0, 0, FIRST + EVERY * (h - 1) + 2))
        kv_arrived(h)

        def query_block(iq, k_now):
            b, final = 2 + per * (h + 1), iq == steps - 1
            k_now = until(k_now, jnp.where(final, complete(b), 0))
            pl.when(final & (h + 1 < kvh))(lambda: load(b, 0, wq_ref, b - 2))
            pl.when(final & (h + 1 == kvh))(lambda: load(b, 0, wo_ref, 0))
            return attend(h, iq, k_now)

        return lax.fori_loop(0, steps, query_block, k_now)

    k_now = lax.fori_loop(0, kvh, key_head, k_now)

    def x_tile(t, slot):
        return pltpu.make_async_copy(x_ref.at[:, pl.ds(pl.multiple_of(t * TILE, TILE), TILE)], xt_s.at[slot], x_sem.at[slot])

    def y_tile(t, slot):
        return pltpu.make_async_copy(yt_s.at[slot], y_ref.at[:, pl.ds(pl.multiple_of(t * TILE, TILE), TILE)], y_sem.at[slot])

    x_tile(0, 0).start()

    def project(t, k_now):
        slot, b = lax.rem(t, 2), 2 + nq + t
        other = 1 - slot
        k_now = until(k_now, complete(b + 1))

        @pl.when(t + 1 < no)
        def _():
            load(b + 1, other, wo_ref, t + 1)
            x_tile(t + 1, other).start()

        loaded(b, slot, wo_ref, t)
        x_tile(t, slot).wait()
        pl.when(t >= 2)(lambda: y_tile(t - 2, slot).wait())

        def outputs(at):
            y = _dot(o_s[pl.ds(at, CHUNK), :], w_s[slot], 1, 0)
            yt_s[slot, pl.ds(at, CHUNK), :] = (xt_s[slot, pl.ds(at, CHUNK), :].astype(jnp.float32) + y).astype(jnp.bfloat16)

        chunks(outputs)
        y_tile(t, slot).start()
        return k_now

    lax.fori_loop(0, no, project, k_now)
    for t in range(max(no - 2, 0), no):
        y_tile(t, t % 2).wait()
    lax.fori_loop(0, blocks, lambda b, _: sent(b), None)
    lax.fori_loop(0, kvh, lambda h, _: kv_sent(h), None)


def solution(mesh):
    n = mesh.shape["sp"]

    def step(x, gain, wq, wk, wv, wo):
        rows, width = x.shape
        part = wq.shape[0]
        kvh = wk.shape[1] // HEAD
        g = wq.shape[1] // wk.shape[1]
        nq, no = wq.shape[1] // TILE, wo.shape[1] // TILE
        blocks = 2 + nq + no
        half = HEAD // 2
        place = lax.axis_index("sp") * rows + jnp.arange(rows)
        lane = jnp.arange(HEAD)
        angle = place.astype(jnp.float32)[:, None] * THETA ** (-(lane % half).astype(jnp.float32) / half)
        cos, sin = jnp.cos(angle), jnp.where(lane < half, -1.0, 1.0) * jnp.sin(angle)
        bf, f32 = jnp.bfloat16, jnp.float32
        hbm, vmem = pl.BlockSpec(memory_space=pl.ANY), pl.BlockSpec(memory_space=pltpu.VMEM)
        dma = pltpu.SemaphoreType.DMA
        y, _ = pl.pallas_call(
            functools.partial(_kernel, n, nq, no, g),
            out_shape=[jax.ShapeDtypeStruct((rows, width), bf), jax.ShapeDtypeStruct((blocks, n * part, TILE), bf)],
            in_specs=[hbm, vmem, vmem, vmem, hbm, hbm, hbm, hbm],
            out_specs=[hbm, hbm],
            scratch_shapes=[
                pltpu.VMEM((rows, width), bf),
                pltpu.VMEM((rows, width), bf),
                pltpu.VMEM((kvh, 2, n * rows, HEAD), bf),
                pltpu.VMEM((2, n * part, TILE), bf),
                pltpu.VMEM((rows, g * HEAD), bf),
                pltpu.VMEM((g, HEAD + 8, BQ), f32),
                pltpu.VMEM((g, BQ), f32),
                pltpu.VMEM((BK, BQ), jnp.int32),
                pltpu.VMEM((2, rows, TILE), bf),
                pltpu.VMEM((2, rows, TILE), bf),
                dma((blocks, 13)),
                dma((blocks, 13)),
                dma((kvh, 4)),
                dma((kvh, 4)),
                dma((2, n)),
                dma((2,)),
                dma((2,)),
                dma,
            ],
            compiler_params=pltpu.CompilerParams(collective_id=0, has_side_effects=True, vmem_limit_bytes=63 * 2**20, flags=FLAGS),
        )(x, gain, cos, sin, wq, wk, wv, wo)
        return y

    tokens, whole = P(("dp", "sp"), None), P("sp", None)
    return jax.shard_map(
        step,
        mesh=mesh,
        in_specs=(tokens, P(None), whole, whole, whole, whole),
        out_specs=tokens,
        check_vma=False,
    )
```

```python
import functools

import jax
import jax.numpy as jnp
from jax import lax
from jax.experimental import pallas as pl
from jax.experimental.pallas import tpu as pltpu
from jax.sharding import PartitionSpec as P

HEAD = 128
THETA = 10000
NEG = -1e30
HIDDEN = 2 * NEG
LOG2E = 1.4426950408889634
TILE = 512
CHUNK = 1024
SMALL = 512
BQ = 512
BK = 512
SEG = 8
MESH = pl.DeviceIdType.MESH
FLAGS = {}
AHEAD = 2
EVERY = 4
RING_BUSY = 8.5
RING_FREE = 10


def _dot(a, b, ca, cb):
    return lax.dot_general(a, b, (((ca,), (cb,)), ((), ())), preferred_element_type=jnp.float32)


def _kernel(n, nq, no, g, x_ref, gain_ref, cos_ref, sin_ref, wq_ref, wk_ref, wv_ref, wo_ref, y_ref, full_ref,
            a_s, o_s, kv_s, w_s, q_s, mix_s, top_s, gap_s, xt_s, yt_s,
            send, recv, kv_send, kv_recv, load_sem, x_sem, y_sem, in_sem):
    me, dp = lax.axis_index("sp"), lax.axis_index("dp")
    rows = x_ref.shape[0]
    part = wq_ref.shape[0]
    kvh = kv_s.shape[0]
    blocks = 2 + nq + no
    right, left, far = lax.rem(me + 1, n), lax.rem(me + n - 1, n), lax.rem(me + 2, n)
    core, pair = lax.rem(dp, 2), lax.rem(lax.div(dp, 2), 2)
    at_right, at_left = {"sp": right}, {"sp": left}
    at_core, at_pair = {"dp": dp + 1 - 2 * core}, {"dp": dp + 2 - 4 * pair}
    origins = (left, right, far)

    barrier = pltpu.get_barrier_semaphore()
    for there in (at_right, at_left, at_core, at_pair):
        pl.semaphore_signal(barrier, inc=1, device_id=there, device_id_type=MESH)
    x_in = pltpu.make_async_copy(x_ref, o_s, in_sem)
    x_in.start()
    pl.semaphore_wait(barrier, 4)

    base, half_part = core * (part // 2), part // 2

    def modes(b):
        busy = (b >= 4) & (b < 2 + nq + 3)
        narrow = b == blocks - 1
        return ((busy, int(RING_BUSY * half_part) // 16), (narrow, half_part),
                (jnp.logical_not(busy | narrow), int(RING_FREE * half_part) // 16))

    def copy(b, i, src, dst, there):
        return pltpu.make_async_remote_copy(src_ref=src, dst_ref=dst, send_sem=send.at[b, i], recv_sem=recv.at[b, i],
                                            device_id=there, device_id_type=MESH)

    def there_and_here(b, i, ref, there):
        return copy(b, i, ref, ref, there)

    def rows_of(b, origin, start, count):
        return full_ref.at[b, pl.ds(pl.multiple_of(origin * part + start, 8), count), :]

    def both(b, do):
        for when, count in modes(b):
            @pl.when(when)
            def _():
                theirs = half_part - count
                do(count, base + pair * theirs, theirs)

    def stage0(b):
        def do(count, start, theirs):
            def go(src, col):
                own = src.at[pl.ds(pl.multiple_of(start, 8), count), pl.ds(pl.multiple_of(col * TILE, TILE), TILE)]
                copy(b, 0, own, rows_of(b, me, start, count), at_right).start()
                copy(b, 1, own, rows_of(b, me, start, count), at_left).start()

            pl.when(b == 0)(lambda: go(wk_ref, 0))
            pl.when(b == 1)(lambda: go(wv_ref, 0))
            pl.when((b >= 2) & (b < 2 + nq))(lambda: go(wq_ref, b - 2))
            pl.when(b >= 2 + nq)(lambda: go(wo_ref, b - 2 - nq))

        both(b, do)

    def onward(b, k, start, count, theirs):
        if theirs:
            there_and_here(b, 4 + k, rows_of(b, origins[k], base + pair * count, theirs), at_pair).start()
        there_and_here(b, 7 + k, rows_of(b, origins[k], start, count), at_core).start()

    def stage1(b):
        def do(count, start, theirs):
            half = count // 2
            there_and_here(b, 0, rows_of(b, left, start, count), at_right).wait_recv()
            there_and_here(b, 2, rows_of(b, left, start, half), at_right).start()
            onward(b, 0, start, count, theirs)
            there_and_here(b, 1, rows_of(b, right, start, count), at_left).wait_recv()
            there_and_here(b, 3, rows_of(b, right, start + half, half), at_left).start()
            onward(b, 1, start, count, theirs)

        both(b, do)

    def stage2(b):
        def do(count, start, theirs):
            half = count // 2
            there_and_here(b, 2, rows_of(b, far, start, half), at_right).wait_recv()
            there_and_here(b, 3, rows_of(b, far, start + half, half), at_left).wait_recv()
            onward(b, 2, start, count, theirs)

        both(b, do)

    def stage3(b):
        def do(count, start, theirs):
            if theirs:
                for k, origin in enumerate(origins):
                    ref = rows_of(b, origin, base + (1 - pair) * count, theirs)
                    there_and_here(b, 4 + k, ref, at_pair).wait_recv()
                    there_and_here(b, 10 + k, ref, at_core).start()

        both(b, do)

    def arrived(b):
        def do(count, _, theirs):
            for k, origin in enumerate(origins):
                there_and_here(b, 7 + k, rows_of(b, origin, 0, count), at_core).wait_recv()
                if theirs:
                    there_and_here(b, 10 + k, rows_of(b, origin, 0, theirs), at_core).wait_recv()

        both(b, do)

    def sent(b):
        def do(count, _, theirs):
            half = count // 2
            sizes = {0: count, 1: count, 2: half, 3: half, 7: count, 8: count, 9: count}
            if theirs:
                sizes |= {4: theirs, 5: theirs, 6: theirs, 10: theirs, 11: theirs, 12: theirs}
            for i, size in sizes.items():
                there_and_here(b, i, rows_of(b, me, 0, size), at_right).wait_send()

        both(b, do)

    def kv_copy(h, i, ref, there):
        return pltpu.make_async_remote_copy(src_ref=ref, dst_ref=ref, send_sem=kv_send.at[h, i], recv_sem=kv_recv.at[h, i],
                                            device_id=there, device_id_type=MESH)

    def kv_at(h, origin, which=None):
        span = pl.ds(pl.multiple_of(origin * rows, 128), rows)
        return kv_s.at[h, :, span, :] if which is None else kv_s.at[h, which, span, :]

    def kv_stage0(h):
        kv_copy(h, 0, kv_at(h, me), at_right).start()
        kv_copy(h, 1, kv_at(h, me), at_left).start()

    def kv_stage1(h):
        kv_copy(h, 0, kv_at(h, left), at_right).wait_recv()
        kv_copy(h, 2, kv_at(h, left, 0), at_right).start()
        kv_copy(h, 1, kv_at(h, right), at_left).wait_recv()
        kv_copy(h, 3, kv_at(h, right, 1), at_left).start()

    def kv_arrived(h):
        kv_copy(h, 2, kv_at(h, far, 0), at_right).wait_recv()
        kv_copy(h, 3, kv_at(h, far, 1), at_left).wait_recv()

    def kv_sent(h):
        for i in range(2):
            kv_copy(h, i, kv_at(h, me), at_right).wait_send()
        for i in range(2):
            kv_copy(h, 2 + i, kv_at(h, me, 0), at_right).wait_send()

    FIRST = 4
    last = blocks + 2

    def tick(k):
        pl.when((k - 2 >= FIRST) & (k - 2 < blocks))(lambda: stage3(k - 2))
        pl.when((k - 1 >= FIRST) & (k - 1 < blocks))(lambda: stage2(k - 1))
        pl.when(k < blocks)(lambda: stage1(k))
        h, at = lax.div(k - FIRST, EVERY) + 1, lax.rem(k - FIRST, EVERY)
        pl.when((h < kvh) & (at == 1))(lambda: kv_stage1(h))
        pl.when((h < kvh) & (at == 0))(lambda: kv_stage0(h))
        pl.when(k + AHEAD < blocks)(lambda: stage0(k + AHEAD))

    def complete(b):
        return jnp.where(b < FIRST, 0, b + 3)

    def turn(k):
        pl.when(k < last)(lambda: tick(k))
        return jnp.minimum(k + 1, last)

    def until(k, target):
        target = jnp.minimum(target, last)
        lax.fori_loop(k, target, lambda i, _: tick(i), None)
        return jnp.maximum(k, target)

    def loads(b, slot, src, col, do):
        for o in range(n):
            into = w_s.at[slot, pl.ds(o * part, part), :]

            @pl.when(me == o)
            def _():
                own = src.at[:, pl.ds(pl.multiple_of(col * TILE, TILE), TILE)]
                do(pltpu.make_async_copy(own, into, load_sem.at[slot, o]))

            @pl.when(me != o)
            def _():
                do(pltpu.make_async_copy(full_ref.at[b, pl.ds(o * part, part), :], into, load_sem.at[slot, o]))

    def load(b, slot, src, col):
        arrived(b)
        loads(b, slot, src, col, lambda c: c.start())

    def loaded(b, slot, src, col):
        loads(b, slot, src, col, lambda c: c.wait())

    for b in range(AHEAD):
        stage0(b)
    gap_s[...] = lax.broadcasted_iota(jnp.int32, gap_s.shape, 1) - lax.broadcasted_iota(jnp.int32, gap_s.shape, 0)
    x_in.wait()

    @pl.loop(0, rows // 64)
    def _(i):
        at = pl.ds(pl.multiple_of(i * 64, 64), 64)
        wide = o_s[at, :].astype(jnp.float32)
        scale = lax.rsqrt(jnp.mean(wide * wide, -1, keepdims=True) + 1e-6)
        a_s[at, :] = (wide * scale * gain_ref[...].astype(jnp.float32)[None]).astype(jnp.bfloat16)

    def chunks(body, size=CHUNK):
        @pl.loop(0, rows // size)
        def _(m):
            body(pl.multiple_of(m * size, size))

    def turned(t, at):
        cos, sin = cos_ref[pl.ds(at, t.shape[0]), :], sin_ref[pl.ds(at, t.shape[0]), :]
        out = []
        for i in range(TILE // HEAD):
            w = t[:, i * HEAD : (i + 1) * HEAD].astype(jnp.float32)
            out.append((w * cos + pltpu.roll(w, HEAD // 2, 1) * sin).astype(jnp.bfloat16))
        return out

    def keys(at):
        t = _dot(a_s[pl.ds(at, SMALL), :], w_s[0], 1, 0).astype(jnp.bfloat16)
        for i, head in enumerate(turned(t, at)):
            kv_s[i, 0, pl.ds(pl.multiple_of(me * rows + at, SMALL), SMALL), :] = head

    def values(at):
        t = _dot(a_s[pl.ds(at, SMALL), :], w_s[1], 1, 0).astype(jnp.bfloat16)
        for i in range(kvh):
            kv_s[i, 1, pl.ds(pl.multiple_of(me * rows + at, SMALL), SMALL), :] = t[:, i * HEAD : (i + 1) * HEAD]

    stage1(0)
    stage0(2)
    stage2(0)
    stage1(1)
    stage0(3)
    stage3(0)
    load(0, 0, wk_ref, 0)
    stage2(1)
    loaded(0, 0, wk_ref, 0)
    chunks(keys, SMALL)
    stage3(1)
    load(1, 1, wv_ref, 0)
    stage1(2)
    loaded(1, 1, wv_ref, 0)
    chunks(values, SMALL)
    kv_stage0(0)
    stage2(2)
    stage1(3)
    stage3(2)
    load(2, 0, wq_ref, 0)
    kv_stage1(0)
    stage0(4)
    stage2(3)
    stage0(5)
    stage3(3)
    k_now = jnp.int32(FIRST)

    per = nq // kvh
    heads = TILE // HEAD
    e = HEAD**-0.5 * LOG2E

    def attend(h, iq, k_now):
        at_q = pl.ds(pl.multiple_of(iq * BQ, BQ), BQ)
        for i in range(g):
            top_s[i : i + 1, :] = jnp.full((1, BQ), NEG, jnp.float32)
            mix_s[i] = jnp.zeros((HEAD + 8, BQ), jnp.float32)
        ones = jnp.ones((8, BK), jnp.bfloat16)

        def block(j, masked):
            at_k = pl.ds(pl.multiple_of(j * BK, BK), BK)
            k = kv_s[h, 0, at_k, :]
            v = jnp.concatenate([kv_s[h, 1, at_k, :].T, ones], axis=0)
            def score(i):
                return _dot(k, q_s[at_q, i * HEAD : (i + 1) * HEAD], 1, 1)

            def weigh(i, s):
                if masked:
                    s = jnp.where(gap_s[...] >= 0, s, HIDDEN)
                old = top_s[i : i + 1, :]
                top = jnp.maximum(old, s.max(axis=0, keepdims=True))
                top_s[i : i + 1, :] = top
                return jnp.exp2((s - top) * e).astype(jnp.bfloat16), jnp.exp2((old - top) * e)

            def mix(i, p, keep):
                mix_s[i] = mix_s[i] * keep + _dot(v, p, 1, 0)

            scores = [score(i) for i in range(g)]
            weights = [weigh(i, s) for i, s in enumerate(scores)]
            for i in range(g):
                mix(i, *weights[i])

        whole = lax.div(me * rows, BK) + iq

        def segment(i, k_now):
            lax.fori_loop(i * SEG, jnp.minimum((i + 1) * SEG, whole), lambda j, _: block(j, False), None)
            return turn(k_now)

        k_now = lax.fori_loop(0, lax.div(whole + SEG - 1, SEG), segment, k_now)
        block(whole, True)
        for i in range(g):
            total = mix_s[i, HEAD : HEAD + 1, :]
            out = (mix_s[i, :HEAD, :] * (1 / total)).T.astype(jnp.bfloat16)
            o_s[at_q, pl.ds(pl.multiple_of(h * g * HEAD + i * HEAD, HEAD), HEAD)] = out
        return k_now

    steps = rows // BQ

    def key_head(h, k_now):
        def query_tile(t, k_now):
            b, slot = 2 + per * h + t, lax.rem(t, 2)
            k_now = until(k_now, jnp.where(t + 1 < per, complete(b + 1), 0))
            pl.when(t + 1 < per)(lambda: load(b + 1, 1 - slot, wq_ref, b - 1))
            loaded(b, slot, wq_ref, b - 2)

            def queries(at):
                out = turned(_dot(a_s[pl.ds(at, CHUNK), :], w_s[slot], 1, 0).astype(jnp.bfloat16), at)
                for i in range(heads):
                    q_s[pl.ds(at, CHUNK), pl.ds(pl.multiple_of((t * heads + i) * HEAD, HEAD), HEAD)] = out[i]

            chunks(queries)
            return k_now

        k_now = lax.fori_loop(0, per, query_tile, k_now)
        k_now = turn(k_now)
        k_now = until(k_now, jnp.where(h == 0, 0, FIRST + EVERY * (h - 1) + 2))
        kv_arrived(h)

        def query_block(iq, k_now):
            b, final = 2 + per * (h + 1), iq == steps - 1
            k_now = until(k_now, jnp.where(final, complete(b), 0))
            pl.when(final & (h + 1 < kvh))(lambda: load(b, 0, wq_ref, b - 2))
            pl.when(final & (h + 1 == kvh))(lambda: load(b, 0, wo_ref, 0))
            return attend(h, iq, k_now)

        return lax.fori_loop(0, steps, query_block, k_now)

    k_now = lax.fori_loop(0, kvh, key_head, k_now)

    def x_tile(t, slot):
        return pltpu.make_async_copy(x_ref.at[:, pl.ds(pl.multiple_of(t * TILE, TILE), TILE)], xt_s.at[slot], x_sem.at[slot])

    def y_tile(t, slot):
        return pltpu.make_async_copy(yt_s.at[slot], y_ref.at[:, pl.ds(pl.multiple_of(t * TILE, TILE), TILE)], y_sem.at[slot])

    x_tile(0, 0).start()

    def project(t, k_now):
        slot, b = lax.rem(t, 2), 2 + nq + t
        other = 1 - slot
        k_now = until(k_now, complete(b + 1))

        @pl.when(t + 1 < no)
        def _():
            load(b + 1, other, wo_ref, t + 1)
            x_tile(t + 1, other).start()

        loaded(b, slot, wo_ref, t)
        x_tile(t, slot).wait()
        pl.when(t >= 2)(lambda: y_tile(t - 2, slot).wait())

        def outputs(at):
            y = _dot(o_s[pl.ds(at, CHUNK), :], w_s[slot], 1, 0)
            yt_s[slot, pl.ds(at, CHUNK), :] = (xt_s[slot, pl.ds(at, CHUNK), :].astype(jnp.float32) + y).astype(jnp.bfloat16)

        chunks(outputs)
        y_tile(t, slot).start()
        return k_now

    lax.fori_loop(0, no, project, k_now)
    for t in range(max(no - 2, 0), no):
        y_tile(t, t % 2).wait()
    lax.fori_loop(0, blocks, lambda b, _: sent(b), None)
    lax.fori_loop(0, kvh, lambda h, _: kv_sent(h), None)


def solution(mesh):
    n = mesh.shape["sp"]

    def step(x, gain, wq, wk, wv, wo):
        rows, width = x.shape
        part = wq.shape[0]
        kvh = wk.shape[1] // HEAD
        g = wq.shape[1] // wk.shape[1]
        nq, no = wq.shape[1] // TILE, wo.shape[1] // TILE
        blocks = 2 + nq + no
        half = HEAD // 2
        place = lax.axis_index("sp") * rows + jnp.arange(rows)
        lane = jnp.arange(HEAD)
        angle = place.astype(jnp.float32)[:, None] * THETA ** (-(lane % half).astype(jnp.float32) / half)
        cos, sin = jnp.cos(angle), jnp.where(lane < half, -1.0, 1.0) * jnp.sin(angle)
        bf, f32 = jnp.bfloat16, jnp.float32
        hbm, vmem = pl.BlockSpec(memory_space=pl.ANY), pl.BlockSpec(memory_space=pltpu.VMEM)
        dma = pltpu.SemaphoreType.DMA
        y, _ = pl.pallas_call(
            functools.partial(_kernel, n, nq, no, g),
            out_shape=[jax.ShapeDtypeStruct((rows, width), bf), jax.ShapeDtypeStruct((blocks, n * part, TILE), bf)],
            in_specs=[hbm, vmem, vmem, vmem, hbm, hbm, hbm, hbm],
            out_specs=[hbm, hbm],
            scratch_shapes=[
                pltpu.VMEM((rows, width), bf),
                pltpu.VMEM((rows, width), bf),
                pltpu.VMEM((kvh, 2, n * rows, HEAD), bf),
                pltpu.VMEM((2, n * part, TILE), bf),
                pltpu.VMEM((rows, g * HEAD), bf),
                pltpu.VMEM((g, HEAD + 8, BQ), f32),
                pltpu.VMEM((g, BQ), f32),
                pltpu.VMEM((BK, BQ), jnp.int32),
                pltpu.VMEM((2, rows, TILE), bf),
                pltpu.VMEM((2, rows, TILE), bf),
                dma((blocks, 13)),
                dma((blocks, 13)),
                dma((kvh, 4)),
                dma((kvh, 4)),
                dma((2, n)),
                dma((2,)),
                dma((2,)),
                dma,
            ],
            compiler_params=pltpu.CompilerParams(collective_id=0, has_side_effects=True, vmem_limit_bytes=63 * 2**20, flags=FLAGS),
        )(x, gain, cos, sin, wq, wk, wv, wo)
        return y

    tokens, whole = P(("dp", "sp"), None), P("sp", None)
    return jax.shard_map(
        step,
        mesh=mesh,
        in_specs=(tokens, P(None), whole, whole, whole, whole),
        out_specs=tokens,
        check_vma=False,
    )
```
